32 devices in a mesh: row: 16 (over z, y, x), col: 2 (over core).
Axes of the slice: x: 2, y: 2, z: 4, core: 2. Of those that a mesh axis runs over, the one named last changes fastest.
Arguments:
- matrix: float32 [3072, 3072], P('row', 'col'), may hold values from -2 to 2, as said below
- diagonal: float32 [3072], P(('row', 'col')), may hold values from 1 to 6
- start: float32 [3072], P(('row', 'col')), may hold values from -6 to 6
Outputs:
- basis: float32 [4, 3072], P(None, ('row', 'col'))
- coefficients: float32 [2, 3], replicated
The draws below stay inside these ranges and needn't reach their ends.
Inputs may be any that keep to these rules, and one draw needn't show every extreme that they name: matrix is exactly symmetric, its entries of order one over the square root of 3072.
All inputs are finite; a program needn't handle non-finite values.
Results may differ from the reference program's by a relative error of at most 0.0003.
Values sent between devices are 32-bit elements.
A program may use at most 64 MiB of HBM per device.

```python
import math
import jax
import jax.numpy as jnp
from jax import lax

ITERS = 3
DIM = 3072


def draw_matrix(key, part):
    raw_draw = jax.random.normal(key, (DIM, DIM), jnp.float32)
    return (raw_draw + raw_draw.T) * (1.0 / math.sqrt(2.0 * DIM))


def steps_of(key, extent, cuts, low, high):
    def one(position, shards_of):
        heights = jax.random.uniform(jax.random.fold_in(jax.random.fold_in(key, 6), position), (shards_of,), jnp.float32, low / len(cuts), high / len(cuts))
        return jnp.repeat(jnp.exp(heights), extent[position] // shards_of).reshape((-1,) + (1,) * (len(extent) - position - 1))

    level = one(*cuts[0])
    for cut in cuts[1:]:
        level = level * one(*cut)
    return level


def bell_draw(rng, dims, scale, most, cuts=(), dtype=jnp.bfloat16):
    array = scale * jax.random.normal(rng, dims, jnp.float32)
    if cuts:
        array = array * steps_of(rng, dims, cuts, -0.22, 0.18)
    return jnp.clip(array, -most, most).astype(dtype)


def setup_inputs(seed: int = 0) -> dict:
    streams_of = jax.random.split(jax.random.key(seed), 4)
    return {
        "matrix": draw_matrix(jax.random.fold_in(streams_of[3], 71), 0),
        "diagonal": jnp.clip(jnp.exp(math.log(6.0) - 1.7917595 * jax.random.uniform(streams_of[1], (DIM,), jnp.float32) ** steps_of(streams_of[1], (DIM,), ((0, 32),), -0.2, 0.2)), 1.0, 6.0),
        "start": bell_draw(streams_of[2], (DIM,), 1.0, 6.0, ((0, 32),), jnp.float32),
    }


def reference(matrix, diagonal, start):
    full_dim = start.shape[0]
    current = start / jnp.sqrt(jnp.sum(start * start))
    basis_rows = jnp.zeros((ITERS + 1, full_dim), jnp.float32).at[0].set(current)
    alpha_list = []
    beta_list = []
    for iteration in range(ITERS):
        image = jnp.dot(matrix, current, precision=lax.Precision.HIGHEST, preferred_element_type=jnp.float32) + diagonal * current
        intersect = jnp.dot(basis_rows, image, precision=lax.Precision.HIGHEST, preferred_element_type=jnp.float32)
        image = image - jnp.dot(intersect, basis_rows, precision=lax.Precision.HIGHEST, preferred_element_type=jnp.float32)
        beta_value = jnp.sqrt(jnp.sum(image * image))
        current = image / beta_value
        basis_rows = basis_rows.at[iteration + 1].set(current)
        alpha_list.append(intersect[iteration])
        beta_list.append(beta_value)
    coefficients = jnp.stack([jnp.stack(alpha_list), jnp.stack(beta_list)])
    return (basis_rows * jnp.sqrt(jnp.float32(full_dim)), coefficients)
```

```python
import functools
import math

import jax
import jax.numpy as jnp
from jax import lax
from jax.experimental import pallas as pl
from jax.experimental.pallas import tpu as pltpu
from jax.sharding import PartitionSpec as P

ITERS = 3
LANES = 128
MESH = pl.DeviceIdType.MESH


class Plan:
    def __init__(self, rows, cols, block, width, chunk):
        self.rows, self.cols, self.block, self.width, self.chunk = rows, cols, block, width, chunk
        self.devices = rows * cols
        self.group = LANES // math.gcd(block, LANES)
        self.tiles = self.group * block // LANES
        self.groups = rows // self.group
        self.bases = [p * block // LANES for p in range(self.group)]
        self.heights = [-(-(p * block % LANES + block) // LANES) for p in range(self.group)]
        self.height = max(self.heights)
        self.col_groups = width // (self.group * block)
        assert rows % self.group == 0 and width % (self.group * block) == 0
        assert chunk * cols == block


def kernel(plan, m_hbm, d_ref, s_ref, basis_ref, coef_ref, m_ref, send, recv, full, m_sem, send_sem, recv_sem):
    n, height, tiles, groups = plan.devices, plan.height, plan.tiles, plan.groups
    row, col = lax.axis_index("row"), lax.axis_index("col")
    me = row * plan.cols + col
    part = lax.rem(row, plan.group)
    offset = lax.rem(part * plan.block, LANES)
    base = (part * plan.block) // LANES
    my_group = row // plan.group

    m_copy = pltpu.make_async_copy(
        m_hbm, m_ref.at[pl.ds(pl.multiple_of(offset, 8), plan.block), :], m_sem
    )
    m_copy.start()

    barrier = pltpu.get_barrier_semaphore()
    peers = []
    for step in range(1, n):
        other = lax.rem(me + step, n)
        peers.append((other // plan.cols, lax.rem(other, plan.cols)))
    for peer in peers:
        pl.semaphore_signal(barrier, inc=1, device_id=peer, device_id_type=MESH)

    def spread(chunk):
        wide = jnp.concatenate(
            [chunk, jnp.zeros((1, height * LANES - plan.chunk), jnp.float32)], axis=1
        )
        return pltpu.roll(wide, offset + col * plan.chunk, 1)

    diagonal = spread(d_ref[...])
    first = spread(s_ref[...])
    lane = lax.broadcasted_iota(jnp.int32, (1, height * LANES), 1)
    inside = (lane >= offset) & (lane < offset + plan.block)

    def post(phase, value):
        for h in range(height):
            tile = value[:, h * LANES : (h + 1) * LANES]
            send[phase, pl.ds(h, 1), :] = tile
            recv[phase, me, pl.ds(h, 1), :] = tile

    def start(phase):
        for peer in peers:
            pltpu.make_async_remote_copy(
                src_ref=send.at[phase],
                dst_ref=recv.at[phase, me],
                send_sem=send_sem.at[phase],
                recv_sem=recv_sem.at[phase],
                device_id=peer,
                device_id_type=MESH,
            ).start()

    def bulk(sem):
        def wait(phase):
            region = recv.at[phase, pl.ds(0, n - 1)]
            pltpu.make_async_copy(region, region, sem.at[phase]).wait()

        return wait

    wait_recv, wait_send = bulk(recv_sem), bulk(send_sem)

    def collect(phase):
        out = [None] * tiles
        for p in range(plan.group):
            for h in range(plan.heights[p]):
                for c in range(plan.cols):
                    value = recv[
                        phase, pl.ds(p * plan.cols + c, groups, stride=plan.group * plan.cols), h, :
                    ]
                    k = plan.bases[p] + h
                    out[k] = value if out[k] is None else out[k] + value
        return out

    def total(values):
        acc = values[0]
        for value in values[1:]:
            acc = acc + value
        return jnp.sum(acc, axis=(0, 1), keepdims=True)

    def keep(index, values):
        for k in range(tiles):
            full[index, k] = values[k]

    def product(index):
        begin = col * plan.col_groups
        partial = []
        for h in range(height):
            acc = None
            for g in range(plan.col_groups):
                for k in range(tiles):
                    t = g * tiles + k
                    v = full[index, k, pl.ds(begin + g, 1), :]
                    term = m_ref[pl.ds(h * LANES, LANES), pl.ds(t * LANES, LANES)] * v
                    acc = term if acc is None else acc + term
            partial.append(jnp.sum(acc.T, axis=0, keepdims=True))
        value = jnp.where(inside, jnp.concatenate(partial, axis=1), 0.0)
        mine = jnp.concatenate(
            [
                full[index, jnp.minimum(base + h, tiles - 1), pl.ds(my_group, 1), :]
                for h in range(height)
            ],
            axis=1,
        )
        return value + diagonal * mine

    scale = math.sqrt(plan.rows * plan.block)
    place = me * plan.chunk
    t0 = place // LANES
    t1 = jnp.minimum(t0 + 1, tiles * groups - 1)
    shift = lax.rem(2 * LANES - lax.rem(place, LANES), 2 * LANES)

    def emit(index):
        pair = [full[index, lax.rem(t, tiles), pl.ds(t // tiles, 1), :] for t in (t0, t1)]
        value = pltpu.roll(jnp.concatenate(pair, axis=1), shift, 1)
        basis_ref[pl.ds(index, 1), :] = value[:, : plan.chunk] * scale

    post(0, first)
    pl.semaphore_wait(barrier, n - 1)
    start(0)
    wait_recv(0)
    values = collect(0)
    inverse = 1.0 / jnp.sqrt(total([v * v for v in values]))
    rows_q = [[v * inverse for v in values]]
    keep(0, rows_q[0])
    alphas, betas = [], []
    m_copy.wait()
    for k in range(ITERS):
        post(k + 1, product(k))
        start(k + 1)
        emit(k)
        wait_recv(k + 1)
        values = collect(k + 1)
        h = [total([a * b for a, b in zip(values, q)]) for q in rows_q]
        for value, q in zip(h, rows_q):
            values = [a - value * b for a, b in zip(values, q)]
        beta = jnp.sqrt(total([a * a for a in values]))
        inverse = 1.0 / beta
        rows_q.append([a * inverse for a in values])
        keep(k + 1, rows_q[-1])
        alphas.append(h[k])
        betas.append(beta)
    emit(ITERS)
    coef_ref[...] = jnp.concatenate(
        [jnp.concatenate(alphas, axis=1), jnp.concatenate(betas, axis=1)], axis=0
    )
    for phase in range(ITERS + 1):
        wait_send(phase)


def per_device(plan, matrix, diagonal, start):
    chunk = plan.chunk
    n, phases = plan.devices, ITERS + 1
    vmem = pl.BlockSpec(memory_space=pltpu.VMEM)
    return pl.pallas_call(
        functools.partial(kernel, plan),
        out_shape=(
            jax.ShapeDtypeStruct((phases, chunk), jnp.float32),
            jax.ShapeDtypeStruct((2, ITERS), jnp.float32),
        ),
        in_specs=[pl.BlockSpec(memory_space=pl.ANY), vmem, vmem],
        out_specs=(vmem, vmem),
        scratch_shapes=[
            pltpu.VMEM((plan.height * LANES, plan.width), jnp.float32),
            pltpu.VMEM((phases, plan.height, LANES), jnp.float32),
            pltpu.VMEM((phases, n, plan.height, LANES), jnp.float32),
            pltpu.VMEM((phases, plan.tiles, plan.groups, LANES), jnp.float32),
            pltpu.SemaphoreType.DMA,
            pltpu.SemaphoreType.DMA((phases,)),
            pltpu.SemaphoreType.DMA((phases,)),
        ],
        compiler_params=pltpu.CompilerParams(collective_id=0, has_side_effects=True),
    )(matrix, diagonal.reshape(1, chunk), start.reshape(1, chunk))


def solution(mesh):
    rows, cols = mesh.shape["row"], mesh.shape["col"]

    def run(matrix, diagonal, start):
        plan = Plan(rows, cols, matrix.shape[0], matrix.shape[1], start.shape[0])
        return per_device(plan, matrix, diagonal, start)

    in_specs = (P("row", "col"), P(("row", "col")), P(("row", "col")))
    out_specs = (P(None, ("row", "col")), P())
    return jax.shard_map(run, mesh=mesh, in_specs=in_specs, out_specs=out_specs, check_vma=False)
```

```python
import functools
import math

import jax
import jax.numpy as jnp
from jax import lax
from jax.experimental import pallas as pl
from jax.experimental.pallas import tpu as pltpu
from jax.sharding import PartitionSpec as P

ITERS = 3
LANES = 128
MESH = pl.DeviceIdType.MESH


class Plan:
    def __init__(self, rows, cols, block, width, chunk):
        self.rows, self.cols, self.block, self.width, self.chunk = rows, cols, block, width, chunk
        self.devices = rows * cols
        self.group = LANES // math.gcd(block, LANES)
        self.tiles = self.group * block // LANES
        self.groups = rows // self.group
        self.bases = [p * block // LANES for p in range(self.group)]
        self.heights = [-(-(p * block % LANES + block) // LANES) for p in range(self.group)]
        self.height = max(self.heights)
        self.col_groups = width // (self.group * block)
        assert rows % self.group == 0 and width % (self.group * block) == 0
        assert chunk * cols == block and cols == 2


def kernel(
    plan, m_hbm, d_hbm, s_hbm, basis_ref, coef_ref,
    m_ref, d_ref, s_ref, d_send, d_all, send, first, recv, full, basis,
    m_sem, d_sem, s_sem, m_over, d_over, send_sem, recv_sem,
):
    n, rows, cols = plan.devices, plan.rows, plan.cols
    height, tiles, groups = plan.height, plan.tiles, plan.groups
    row, col = lax.axis_index("row"), lax.axis_index("col")
    me = row * cols + col
    lead = cols - 1
    part = lax.rem(row, plan.group)
    offset = lax.rem(part * plan.block, LANES)
    base = (part * plan.block) // LANES
    my_group = row // plan.group
    wide = height * LANES

    peers = [partner(me, step, n) for step in range(n - 1, 0, -1)]
    peers = [(other // cols, lax.rem(other, cols)) for other in peers]
    barrier = pltpu.get_barrier_semaphore()
    for peer in peers:
        pl.semaphore_signal(barrier, inc=1, device_id=peer, device_id_type=MESH)

    def spread(chunk):
        padded = jnp.concatenate([chunk, jnp.zeros((1, wide - plan.chunk), jnp.float32)], axis=1)
        return pltpu.roll(padded, offset + col * plan.chunk, 1)

    def put(ref, index, value):
        for h in range(height):
            ref[index, pl.ds(h, 1), :] = value[:, h * LANES : (h + 1) * LANES]

    def remote(src, dst, ssem, rsem, peer):
        return pltpu.make_async_remote_copy(
            src_ref=src, dst_ref=dst, send_sem=ssem, recv_sem=rsem, device_id=peer, device_id_type=MESH
        )

    def bulk(count, sem):
        region = first.at[pl.ds(0, count)]
        pltpu.make_async_copy(region, region, sem).wait()

    def gathered(load, count):
        out = [None] * tiles
        for p in range(plan.group):
            for h in range(plan.heights[p]):
                for c in range(count):
                    value = load(p * count + c, plan.group * count, h)
                    k = plan.bases[p] + h
                    out[k] = value if out[k] is None else out[k] + value
        return out

    def total(values):
        acc = values[0]
        for value in values[1:]:
            acc = acc + value
        return jnp.sum(acc, axis=(0, 1), keepdims=True)

    def dot(a, b):
        return total([x * y for x, y in zip(a, b)])

    def store(ref, index, values):
        for k in range(tiles):
            ref[index, k] = values[k]

    def product(index):
        partial = []
        for low in range(0, plan.block, LANES):
            size = min(LANES, plan.block - low)
            acc = None
            for t in range(cols * plan.width // LANES):
                v = full[index, t % tiles, pl.ds(t // tiles, 1), :]
                term = m_ref[pl.ds(low, size), pl.ds(t * LANES, LANES)] * v
                acc = term if acc is None else acc + term
            partial.append(jnp.sum(acc.T, axis=0, keepdims=True))
        if wide > plan.block:
            partial.append(jnp.zeros((1, wide - plan.block), jnp.float32))
        value = pltpu.roll(jnp.concatenate(partial, axis=1), offset, 1)
        mine = jnp.concatenate(
            [
                full[index, jnp.minimum(base + h, tiles - 1), pl.ds(my_group, 1), :]
                for h in range(height)
            ],
            axis=1,
        )
        diagonal = jnp.concatenate(
            [sum(d_all[c, pl.ds(h, 1), :] for c in range(cols)) for h in range(height)], axis=1
        )
        return value + diagonal * mine

    scale = math.sqrt(rows * plan.block)
    place = me * plan.chunk
    t0 = place // LANES
    t1 = jnp.minimum(t0 + 1, tiles * groups - 1)
    shift = lax.rem(2 * LANES - lax.rem(place, LANES), 2 * LANES)

    def emit(index):
        pair = [basis[index, lax.rem(t, tiles), pl.ds(t // tiles, 1), :] for t in (t0, t1)]
        value = pltpu.roll(jnp.concatenate(pair, axis=1), shift, 1)
        basis_ref[pl.ds(index, 1), :] = value[:, : plan.chunk] * scale

    def body(leading):
        half = m_ref.at[:, pl.ds(pl.multiple_of(col * plan.width, LANES), plan.width)]
        copies = [
            pltpu.make_async_copy(s_hbm, s_ref, s_sem),
            pltpu.make_async_copy(d_hbm, d_ref, d_sem),
            pltpu.make_async_copy(m_hbm, half, m_sem),
        ]
        for copy in copies:
            copy.start()
        copies[0].wait()
        value = spread(s_ref[...])
        put(send, 0, value)
        put(first, me, value)
        copies[1].wait()
        put(d_all if leading else d_send, lead if leading else 0, spread(d_ref[...]))
        pl.semaphore_wait(barrier, n - 1)
        for peer in peers:
            remote(send.at[0], first.at[me], send_sem.at[0], recv_sem.at[0], peer).start()
        copies[2].wait()
        over = (
            remote(d_send.at[0], d_all.at[col], d_over.at[0], d_over.at[1], (row, lead)),
            remote(half, half, m_over.at[0], m_over.at[1], (row, lead)),
        )
        if not leading:
            for copy in over:
                copy.start()
        bulk(n - 1, recv_sem.at[0])
        raw = gathered(lambda at, stride, h: first[pl.ds(at, groups, stride=stride), h, :], cols)
        if leading:
            for c in range(lead):
                other = m_ref.at[:, pl.ds(c * plan.width, plan.width)]
                remote(other, other, m_over.at[0], m_over.at[1], (row, c)).wait_recv()
                remote(d_send.at[0], d_all.at[c], d_over.at[0], d_over.at[1], (row, c)).wait_recv()
        q, images, alphas, betas = [], [], [], []
        for k in range(ITERS + 1):
            store(full, k, raw)
            image = product(k) if leading and k < ITERS else None
            h = [dot(raw, other) for other in q]
            rest = raw
            for value, other in zip(h, q):
                rest = [a - value * b for a, b in zip(rest, other)]
            beta = jnp.sqrt(dot(rest, rest))
            inverse = 1.0 / beta
            if k:
                alphas.append(h[k - 1])
                betas.append(beta)
            if image is not None:
                for value, other in zip(h, images):
                    image = image - value * other
                image = image * inverse
                images.append(image)
                put(send, k + 1, image)
                put(recv, k * rows + row, image)
                for peer in peers:
                    remote(
                        send.at[k + 1],
                        recv.at[k * rows + row],
                        send_sem.at[k + 1],
                        recv_sem.at[k + 1],
                        peer,
                    ).start()
            q.append([a * inverse for a in rest])
            store(basis, k, q[-1])
            emit(k)
            if k < ITERS:
                bulk(rows - 1 if leading else rows, recv_sem.at[k + 1])
                raw = gathered(
                    lambda at, stride, h: recv[pl.ds(k * rows + at, groups, stride=stride), h, :], 1
                )
        coef_ref[...] = jnp.concatenate(
            [jnp.concatenate(alphas, axis=1), jnp.concatenate(betas, axis=1)], axis=0
        )
        bulk(n - 1, send_sem.at[0])
        if leading:
            for k in range(ITERS):
                bulk(n - 1, send_sem.at[k + 1])
        else:
            for copy in over:
                copy.wait_send()

    pl.when(col == lead)(lambda: body(True))
    pl.when(col != lead)(lambda: body(False))


def partner(me, step, n):
    if n & (n - 1):
        return lax.rem(me + step, n)
    other, bit = me, 1
    while bit < n:
        if step & bit:
            other = other + bit - 2 * bit * lax.rem(me // bit, 2)
        bit *= 2
    return other


def per_device(plan, matrix, diagonal, start):
    chunk, height = plan.chunk, plan.height
    n, rows, cols, phases = plan.devices, plan.rows, plan.cols, ITERS + 1
    vmem = pl.BlockSpec(memory_space=pltpu.VMEM)
    hbm = pl.BlockSpec(memory_space=pl.ANY)
    f32 = jnp.float32
    return pl.pallas_call(
        functools.partial(kernel, plan),
        out_shape=(
            jax.ShapeDtypeStruct((phases, chunk), f32),
            jax.ShapeDtypeStruct((2, ITERS), f32),
        ),
        in_specs=[hbm, hbm, hbm],
        out_specs=(vmem, vmem),
        scratch_shapes=[
            pltpu.VMEM((plan.block, cols * plan.width), f32),
            pltpu.VMEM((1, chunk), f32),
            pltpu.VMEM((1, chunk), f32),
            pltpu.VMEM((1, height, LANES), f32),
            pltpu.VMEM((cols, height, LANES), f32),
            pltpu.VMEM((phases, height, LANES), f32),
            pltpu.VMEM((n, height, LANES), f32),
            pltpu.VMEM((ITERS * rows, height, LANES), f32),
            pltpu.VMEM((phases, plan.tiles, plan.groups, LANES), f32),
            pltpu.VMEM((phases, plan.tiles, plan.groups, LANES), f32),
            pltpu.SemaphoreType.DMA,
            pltpu.SemaphoreType.DMA,
            pltpu.SemaphoreType.DMA,
            pltpu.SemaphoreType.DMA((2,)),
            pltpu.SemaphoreType.DMA((2,)),
            pltpu.SemaphoreType.DMA((phases,)),
            pltpu.SemaphoreType.DMA((phases,)),
        ],
        compiler_params=pltpu.CompilerParams(collective_id=0, has_side_effects=True),
    )(matrix, diagonal.reshape(1, chunk), start.reshape(1, chunk))


def solution(mesh):
    rows, cols = mesh.shape["row"], mesh.shape["col"]

    def run(matrix, diagonal, start):
        plan = Plan(rows, cols, matrix.shape[0], matrix.shape[1], start.shape[0])
        return per_device(plan, matrix, diagonal, start)

    in_specs = (P("row", "col"), P(("row", "col")), P(("row", "col")))
    out_specs = (P(None, ("row", "col")), P())
    return jax.shard_map(run, mesh=mesh, in_specs=in_specs, out_specs=out_specs, check_vma=False)
```

```python
import functools
import math

import jax
import jax.numpy as jnp
from jax import lax
from jax.experimental import pallas as pl
from jax.experimental.pallas import tpu as pltpu
from jax.sharding import PartitionSpec as P

ITERS = 3
LANES = 128
MESH = pl.DeviceIdType.MESH


class Plan:
    def __init__(self, rows, cols, block, width, chunk):
        self.rows, self.cols, self.block, self.width, self.chunk = rows, cols, block, width, chunk
        self.devices = rows * cols
        self.group = LANES // math.gcd(block, LANES)
        self.tiles = self.group * block // LANES
        self.groups = rows // self.group
        self.bases = [p * block // LANES for p in range(self.group)]
        self.heights = [-(-(p * block % LANES + block) // LANES) for p in range(self.group)]
        self.height = max(self.heights)
        self.col_groups = width // (self.group * block)
        assert rows % self.group == 0 and width % (self.group * block) == 0
        assert chunk * cols == block and cols == 2


def kernel(
    plan, m_hbm, d_hbm, s_hbm, basis_ref, coef_ref,
    m_ref, d_ref, s_ref, d_send, d_all, send, first, recv, full, basis,
    m_sem, d_sem, s_sem, m_over, d_over, send_sem, recv_sem,
):
    n, rows, cols = plan.devices, plan.rows, plan.cols
    height, tiles, groups = plan.height, plan.tiles, plan.groups
    row, col = lax.axis_index("row"), lax.axis_index("col")
    me = row * cols + col
    lead = cols - 1
    part = lax.rem(row, plan.group)
    offset = lax.rem(part * plan.block, LANES)
    base = (part * plan.block) // LANES
    my_group = row // plan.group
    wide = height * LANES

    peers = [partner(me, step, n) for step in range(n - 1, 0, -1)]
    peers = [(other // cols, lax.rem(other, cols)) for other in peers]
    barrier = pltpu.get_barrier_semaphore()
    for peer in peers:
        pl.semaphore_signal(barrier, inc=1, device_id=peer, device_id_type=MESH)

    def spread(chunk):
        padded = jnp.concatenate([chunk, jnp.zeros((1, wide - plan.chunk), jnp.float32)], axis=1)
        return pltpu.roll(padded, offset + col * plan.chunk, 1)

    def put(ref, index, value):
        for h in range(height):
            ref[index, pl.ds(h, 1), :] = value[:, h * LANES : (h + 1) * LANES]

    def remote(src, dst, ssem, rsem, peer):
        return pltpu.make_async_remote_copy(
            src_ref=src, dst_ref=dst, send_sem=ssem, recv_sem=rsem, device_id=peer, device_id_type=MESH
        )

    def bulk(count, sem):
        region = first.at[pl.ds(0, count)]
        pltpu.make_async_copy(region, region, sem).wait()

    def gathered(load, count):
        out = [None] * tiles
        for p in range(plan.group):
            for h in range(plan.heights[p]):
                for c in range(count):
                    value = load(p * count + c, plan.group * count, h)
                    k = plan.bases[p] + h
                    out[k] = value if out[k] is None else out[k] + value
        return out

    def total(values):
        acc = values[0]
        for value in values[1:]:
            acc = acc + value
        return jnp.sum(acc, axis=(0, 1), keepdims=True)

    def dot(a, b):
        return total([x * y for x, y in zip(a, b)])

    def store(ref, index, values):
        for k in range(tiles):
            ref[index, k] = values[k]

    def product(index):
        partial = []
        for low in range(0, plan.block, LANES):
            size = min(LANES, plan.block - low)
            acc = None
            for t in range(cols * plan.width // LANES):
                v = full[index, t % tiles, pl.ds(t // tiles, 1), :]
                term = m_ref[pl.ds(low, size), pl.ds(t * LANES, LANES)] * v
                acc = term if acc is None else acc + term
            partial.append(jnp.sum(acc.T, axis=0, keepdims=True))
        if wide > plan.block:
            partial.append(jnp.zeros((1, wide - plan.block), jnp.float32))
        value = pltpu.roll(jnp.concatenate(partial, axis=1), offset, 1)
        mine = jnp.concatenate(
            [
                full[index, jnp.minimum(base + h, tiles - 1), pl.ds(my_group, 1), :]
                for h in range(height)
            ],
            axis=1,
        )
        diagonal = jnp.concatenate(
            [sum(d_all[c, pl.ds(h, 1), :] for c in range(cols)) for h in range(height)], axis=1
        )
        return value + diagonal * mine

    scale = math.sqrt(rows * plan.block)
    place = me * plan.chunk
    t0 = place // LANES
    t1 = jnp.minimum(t0 + 1, tiles * groups - 1)
    shift = lax.rem(2 * LANES - lax.rem(place, LANES), 2 * LANES)

    def emit(index):
        pair = [basis[index, lax.rem(t, tiles), pl.ds(t // tiles, 1), :] for t in (t0, t1)]
        value = pltpu.roll(jnp.concatenate(pair, axis=1), shift, 1)
        basis_ref[pl.ds(index, 1), :] = value[:, : plan.chunk] * scale

    def body(leading):
        half = m_ref.at[:, pl.ds(pl.multiple_of(col * plan.width, LANES), plan.width)]
        copies = [
            pltpu.make_async_copy(s_hbm, s_ref, s_sem),
            pltpu.make_async_copy(d_hbm, d_ref, d_sem),
            pltpu.make_async_copy(m_hbm, half, m_sem),
        ]
        for copy in copies:
            copy.start()
        copies[0].wait()
        value = spread(s_ref[...])
        put(send, 0, value)
        put(first, me, value)
        copies[1].wait()
        put(d_all if leading else d_send, lead if leading else 0, spread(d_ref[...]))
        pl.semaphore_wait(barrier, n - 1)
        for peer in peers:
            remote(send.at[0], first.at[me], send_sem.at[0], recv_sem.at[0], peer).start()
        copies[2].wait()
        over = (
            remote(d_send.at[0], d_all.at[col], d_over.at[0], d_over.at[1], (row, lead)),
            remote(half, half, m_over.at[0], m_over.at[1], (row, lead)),
        )
        if not leading:
            for copy in over:
                copy.start()
        bulk(n - 1, recv_sem.at[0])
        raw = gathered(lambda at, stride, h: first[pl.ds(at, groups, stride=stride), h, :], cols)
        if leading:
            for c in range(lead):
                other = m_ref.at[:, pl.ds(c * plan.width, plan.width)]
                remote(other, other, m_over.at[0], m_over.at[1], (row, c)).wait_recv()
                remote(d_send.at[0], d_all.at[c], d_over.at[0], d_over.at[1], (row, c)).wait_recv()
        q, images, alphas, betas = [], [], [], []
        for k in range(ITERS + 1):
            store(full, k, raw)
            image = product(k) if leading and k < ITERS else None
            h = [dot(raw, other) for other in q]
            rest = raw
            for value, other in zip(h, q):
                rest = [a - value * b for a, b in zip(rest, other)]
            beta = jnp.sqrt(dot(rest, rest))
            inverse = 1.0 / beta
            if k:
                alphas.append(h[k - 1])
                betas.append(beta)
            if image is not None:
                for value, other in zip(h, images):
                    image = image - value * other
                image = image * inverse
                images.append(image)
                put(send, k + 1, image)
                put(recv, k * rows + row, image)
                for peer in peers:
                    remote(
                        send.at[k + 1],
                        recv.at[k * rows + row],
                        send_sem.at[k + 1],
                        recv_sem.at[k + 1],
                        peer,
                    ).start()
            q.append([a * inverse for a in rest])
            store(basis, k, q[-1])
            emit(k)
            if k < ITERS:
                bulk(rows - 1 if leading else rows, recv_sem.at[k + 1])
                raw = gathered(
                    lambda at, stride, h: recv[pl.ds(k * rows + at, groups, stride=stride), h, :], 1
                )
        coef_ref[...] = jnp.concatenate(
            [jnp.concatenate(alphas, axis=1), jnp.concatenate(betas, axis=1)], axis=0
        )
        bulk(n - 1, send_sem.at[0])
        if leading:
            for k in range(ITERS):
                bulk(n - 1, send_sem.at[k + 1])
        else:
            for copy in over:
                copy.wait_send()

    pl.when(col == lead)(lambda: body(True))
    pl.when(col != lead)(lambda: body(False))


def partner(me, step, n):
    if n & (n - 1):
        return lax.rem(me + step, n)
    other, bit = me, 1
    while bit < n:
        if step & bit:
            other = other + bit - 2 * bit * lax.rem(me // bit, 2)
        bit *= 2
    return other


def per_device(plan, matrix, diagonal, start):
    chunk, height = plan.chunk, plan.height
    n, rows, cols, phases = plan.devices, plan.rows, plan.cols, ITERS + 1
    vmem = pl.BlockSpec(memory_space=pltpu.VMEM)
    hbm = pl.BlockSpec(memory_space=pl.ANY)
    f32 = jnp.float32
    return pl.pallas_call(
        functools.partial(kernel, plan),
        out_shape=(
            pltpu.VMEM((phases, chunk), f32),
            pltpu.VMEM((2, ITERS), f32),
        ),
        in_specs=[hbm, hbm, hbm],
        out_specs=(vmem, vmem),
        scratch_shapes=[
            pltpu.VMEM((plan.block, cols * plan.width), f32),
            pltpu.VMEM((1, chunk), f32),
            pltpu.VMEM((1, chunk), f32),
            pltpu.VMEM((1, height, LANES), f32),
            pltpu.VMEM((cols, height, LANES), f32),
            pltpu.VMEM((phases, height, LANES), f32),
            pltpu.VMEM((n, height, LANES), f32),
            pltpu.VMEM((ITERS * rows, height, LANES), f32),
            pltpu.VMEM((phases, plan.tiles, plan.groups, LANES), f32),
            pltpu.VMEM((phases, plan.tiles, plan.groups, LANES), f32),
            pltpu.SemaphoreType.DMA,
            pltpu.SemaphoreType.DMA,
            pltpu.SemaphoreType.DMA,
            pltpu.SemaphoreType.DMA((2,)),
            pltpu.SemaphoreType.DMA((2,)),
            pltpu.SemaphoreType.DMA((phases,)),
            pltpu.SemaphoreType.DMA((phases,)),
        ],
        compiler_params=pltpu.CompilerParams(collective_id=0, has_side_effects=True),
    )(matrix, diagonal.reshape(1, chunk), start.reshape(1, chunk))


def solution(mesh):
    rows, cols = mesh.shape["row"], mesh.shape["col"]

    def run(matrix, diagonal, start):
        plan = Plan(rows, cols, matrix.shape[0], matrix.shape[1], start.shape[0])
        return per_device(plan, matrix, diagonal, start)

    in_specs = (P("row", "col"), P(("row", "col")), P(("row", "col")))
    out_specs = (P(None, ("row", "col")), P())
    return jax.shard_map(run, mesh=mesh, in_specs=in_specs, out_specs=out_specs, check_vma=False)
```
